256 devices in a mesh: nodes: 64 (over x, z, y_hi), dp: 4 (over y_lo, core).
Axes of the slice: x: 4, y: 4 (y_hi: 2, y_lo: 2; y = y_hi * 2 + y_lo), z: 8, core: 2. Of those that a mesh axis runs over, the one named last changes fastest.
Arguments:
- samples: float32 [16384, 256], P('dp'), may hold values from -96 to 96, as said below
- basis_matrix: float32 [65536, 4096], P('nodes', 'dp'), may hold values from 0 to 0.03
- weights: float32 [4096, 256], P('dp'), may hold values from -12 to 12, as said below
Outputs:
- new_weights: float32 [4096, 256], P('dp')
- new_centres: float32 [65536, 256], P('nodes')
The draws below stay inside these ranges and needn't reach their ends.
Inputs may be any that keep to these rules, and one draw needn't show every extreme that they name: `samples`: finite data values. `weights`: finite weight values.
All inputs are finite; a program needn't handle non-finite values.
Results may differ from the reference program's by a relative error of at most 0.0003.
Values sent between devices are 32-bit elements; how exact they have to be, the bound alone decides.
No kernel may reach another device: no remote copies, remote signals or barrier semaphores. Data moves between devices by JAX's collectives and lax.ppermute only.
A program may use at most 64 MiB of HBM per device.

```python
import math
import jax
import jax.numpy as jnp
from jax import lax

D = 256
M = 4096
KDEV = 1024
K = 65536
N = 16384


def draw_samples(key, part):
    first_key = jax.random.fold_in(jax.random.fold_in(key, 7), 0)
    mask_key, level_key, noise_key = jax.random.split(jax.random.fold_in(key, 13), 3)
    values = jnp.clip(jax.random.normal(first_key, (N, D), jnp.float32), -6.0, 6.0)
    picked = jax.random.uniform(mask_key, (N, 1), jnp.float32) < 0.125
    picked = jnp.logical_or(picked, (jnp.arange(N) == 0)[:, None])
    levels = jax.random.uniform(level_key, (N, 1), jnp.float32, 0.55, 1.0)
    strong = jnp.clip(84.0 * levels + 2.0 * jax.random.normal(noise_key, (N, D), jnp.float32), -96.0, 96.0)
    columns = (jnp.arange(D) < 4)[None, :]
    return jnp.where(jnp.logical_and(picked, columns), strong, values)


def draw_weights(key, part):
    weight_key = jax.random.fold_in(key, 11)
    values = jnp.clip(jax.random.normal(weight_key, (M, D), jnp.float32), -6.0, 6.0)
    values = values - jnp.mean(values, axis=0, keepdims=True)
    shared = jnp.where(jnp.arange(D) < 4, 8.0 / (0.015 * M), 0.0)
    return values + shared[None, :]


def block_scale(rng, extent, cuts, smallest, top_value):
    loudness = 1.0
    for axis_at, shards_of in cuts:
        heights = jax.random.uniform(jax.random.fold_in(jax.random.fold_in(rng, 6), axis_at), (shards_of,), jnp.float32, smallest / len(cuts), top_value / len(cuts))
        loudness = loudness * jnp.repeat(jnp.exp(heights), extent[axis_at] // shards_of).reshape((-1,) + (1,) * (len(extent) - 1 - axis_at))
    return loudness


def setup_inputs(seed: int = 0) -> dict:
    arg_keys = jax.random.split(jax.random.key(seed), 4)
    return {
        "samples": draw_samples(jax.random.fold_in(arg_keys[3], 71), 0),
        "basis_matrix": jnp.clip(0.03 * jax.random.uniform(arg_keys[1], (K, M), jnp.float32) ** block_scale(arg_keys[1], (K, M), ((0, 64), (1, 4)), -0.2, 0.2), 0.0, 0.03),
        "weights": draw_weights(jax.random.fold_in(arg_keys[3], 71), 0),
    }


highest = lax.Precision.HIGHEST
inverse_temp = 0.25
shrink = 0.95

def node_scores(centre_block, samples):
    cross = lax.dot_general(centre_block, samples, (((1,), (1,)), ((), ())), precision=highest, preferred_element_type=jnp.float32)
    return inverse_temp * (cross - 0.5 * lax.optimization_barrier(jnp.sum(centre_block * centre_block, axis=1))[:, None])

def reference(samples, basis_matrix, weights):
    centres = jnp.dot(basis_matrix, weights, precision=highest, preferred_element_type=jnp.float32)
    blocks = centres.reshape(K // KDEV, KDEV, D)

    def update(running, centre_block):
        maxima, totals = running
        scores = node_scores(centre_block, samples)
        merged = jnp.maximum(maxima, lax.optimization_barrier(jnp.max(scores, axis=0)))
        totals = totals * jnp.exp(maxima - merged) + lax.optimization_barrier(jnp.sum(jnp.exp(scores - merged[None, :]), axis=0))
        return ((merged, totals), None)
    start = (jnp.full((N,), -jnp.inf, jnp.float32), jnp.zeros((N,), jnp.float32))
    (maxima, totals), _ = lax.scan(update, start, blocks)

    def terms(centre_block):
        resp = jnp.exp(node_scores(centre_block, samples) - maxima[None, :]) / totals[None, :]
        weighted = jnp.dot(resp, samples, precision=highest, preferred_element_type=jnp.float32)
        return lax.optimization_barrier(jnp.sum(resp, axis=1))[:, None] * centre_block - weighted
    node_terms = lax.map(terms, blocks).reshape(K, D)
    gradient = lax.dot_general(basis_matrix, node_terms, (((0,), (0,)), ((), ())), precision=highest, preferred_element_type=jnp.float32)
    step_rate = 8.0 * math.sqrt(K) / N
    new_weights = shrink * weights - step_rate * gradient
    new_centres = jnp.dot(basis_matrix, new_weights, precision=highest, preferred_element_type=jnp.float32)
    return (new_weights, new_centres)
```

```python
import math

import jax
import jax.numpy as jnp
from jax import lax
from jax.sharding import Mesh
from jax.sharding import PartitionSpec as P

PLANE = ("x", "z")
NODES = ("x", "z", "y_hi")
DP = ("y_lo", "core")
CHUNKS = 4

highest = lax.Precision.HIGHEST
inverse_temp = 0.25
shrink = 0.95


def swapped(array, axis):
    return lax.ppermute(array, axis, [(0, 1), (1, 0)])


def partner(array, axis, distance):
    count = lax.axis_size(axis)
    return lax.ppermute(array, axis, [(k, k ^ distance) for k in range(count)])


def dot(first, second, first_dim=1, second_dim=0):
    return lax.dot_general(
        first,
        second,
        (((first_dim,), (second_dim,)), ((), ())),
        precision=highest,
        preferred_element_type=jnp.float32,
    )


def summed_halves(mine, other):
    chip = mine + swapped(other, "core")
    full = chip + swapped(chip, "y_lo")
    return full, swapped(full, "core")


def merged(first, second):
    top = jnp.maximum(first[0], second[0])
    return jnp.stack(
        [top, first[1] * jnp.exp(first[0] - top) + second[1] * jnp.exp(second[0] - top)]
    )


def over_nodes(stats):
    for axis in NODES:
        distance = 1
        while distance < lax.axis_size(axis):
            stats = merged(stats, partner(stats, axis, distance))
            distance *= 2
    return stats


def body(samples, basis_matrix, weights):
    node_count = basis_matrix.shape[0] * lax.axis_size(NODES)
    vector_count = samples.shape[0] * lax.axis_size(DP)
    core = lax.axis_index("core")
    half = basis_matrix.shape[0] // 2
    rows = half // CHUNKS

    def basis_rows(side, chunk):
        start = (core if side == 0 else 1 - core) * half + chunk * rows
        return lax.dynamic_slice_in_dim(basis_matrix, start, rows, 0)

    blocks = [(basis_rows(0, q), basis_rows(1, q)) for q in range(CHUNKS)]
    centres, scores = [], []
    for own, others in blocks:
        pair = summed_halves(dot(own, weights), dot(others, weights))
        block = jnp.concatenate(pair)
        cross = dot(block, samples, 1, 1)
        centres.append(block)
        scores.append(inverse_temp * (cross - 0.5 * jnp.sum(block * block, axis=1)[:, None]))
    local_max = jnp.max(scores[0], axis=0)
    for part in scores[1:]:
        local_max = jnp.maximum(local_max, jnp.max(part, axis=0))
    exponents = [jnp.exp(part - local_max[None, :]) for part in scores]
    local_total = sum(jnp.sum(part, axis=0) for part in exponents)
    maxima, totals = over_nodes(jnp.stack([local_max, local_total]))
    factor = jnp.exp(local_max - maxima) / totals

    partial_gradient = 0.0
    for (own, others), block, exponent in zip(blocks, centres, exponents):
        resp = exponent * factor[None, :]
        terms = jnp.sum(resp, axis=1)[:, None] * block - dot(resp, samples)
        own_terms, other_terms = summed_halves(terms[:rows], terms[rows:])
        partial_gradient += dot(own, own_terms, 0, 0) + dot(others, other_terms, 0, 0)

    step_rate = 8.0 * math.sqrt(node_count) / vector_count
    count = lax.axis_size(PLANE)
    parts = partial_gradient.reshape(count, -1, partial_gradient.shape[1])
    gradient_rows = lax.all_to_all(parts, PLANE, 0, 0, tiled=True).sum(axis=0)
    gradient_rows = gradient_rows + swapped(gradient_rows, "y_hi")
    row_count = gradient_rows.shape[0]
    own_rows = lax.dynamic_slice_in_dim(weights, lax.axis_index(PLANE) * row_count, row_count, 0)
    updated = shrink * own_rows - step_rate * gradient_rows
    spread = jnp.broadcast_to(updated[None], (count, *updated.shape))
    new_weights = lax.all_to_all(spread, PLANE, 0, 0, tiled=True).reshape(weights.shape)

    own_blocks, other_blocks = [], []
    for own, others in blocks:
        pair = summed_halves(dot(own, new_weights), dot(others, new_weights))
        own_blocks.append(pair[0])
        other_blocks.append(pair[1])
    mine, sibling = jnp.concatenate(own_blocks), jnp.concatenate(other_blocks)
    first = core == 0
    new_centres = jnp.concatenate(
        [jnp.where(first, mine, sibling), jnp.where(first, sibling, mine)]
    )
    return (new_weights, new_centres)


def solution(mesh):
    split = Mesh(mesh.devices.reshape(4, 8, 2, 2, 2), NODES + DP)
    placed = (P(DP, None), P(NODES, DP), P(DP, None))
    return jax.shard_map(
        body,
        mesh=split,
        in_specs=placed,
        out_specs=(P(DP, None), P(NODES, None)),
        check_vma=False,
    )
```

```python
import math

import jax
import jax.numpy as jnp
from jax import lax
from jax.sharding import Mesh
from jax.sharding import PartitionSpec as P


NODES = ("x", "z", "y_hi")
DP = ("y_lo", "core")
CHUNKS = (256, 384, 384)

three_pass = lax.Precision.HIGH
inverse_temp = 0.25
shrink = 0.95


def swapped(array, axis):
    return lax.ppermute(array, axis, [(0, 1), (1, 0)])


def dot(first, second, first_dim=1, second_dim=0, precision=three_pass):
    return lax.dot_general(
        first,
        second,
        (((first_dim,), (second_dim,)), ((), ())),
        precision=precision,
        preferred_element_type=jnp.float32,
    )


def chip_sum(partial):
    half = partial.shape[0] // 2
    first = lax.axis_index("core") == 0
    top, bottom = partial[:half], partial[half:]
    mine, other = jnp.where(first, top, bottom), jnp.where(first, bottom, top)
    return mine + swapped(other, "core")


def whole_sum(chip, arrived):
    first = lax.axis_index("core") == 0
    full = chip + arrived
    sibling = swapped(full, "core")
    return jnp.concatenate([jnp.where(first, full, sibling), jnp.where(first, sibling, full)])


def merged(*stats):
    top = stats[0][0]
    for other in stats[1:]:
        top = jnp.maximum(top, other[0])
    total = sum(other[1] * jnp.exp(other[0] - top) for other in stats)
    return jnp.stack([top, total])


def moved(array, axis, where):
    count = lax.axis_size(axis)
    return lax.ppermute(array, axis, [(k, where(k) % count) for k in range(count)])


def over_nodes(stats):
    others = [moved(stats, "x", lambda k, d=d: k + d) for d in (1, 3, 2)]
    stats = merged(stats, *others)
    for flip in (1, 3, 7):
        stats = merged(stats, moved(stats, "z", lambda k: k ^ flip))
    return merged(stats, swapped(stats, "y_hi"))


def scattered(array, axis):
    parts = array.reshape(lax.axis_size(axis), -1, array.shape[1])
    return lax.all_to_all(parts, axis, 0, 0, tiled=True).sum(axis=0)


def gathered(array, axis):
    spread = jnp.broadcast_to(array[None], (lax.axis_size(axis), *array.shape))
    return lax.all_to_all(spread, axis, 0, 0, tiled=True).reshape(-1, array.shape[1])


def step(samples, basis_matrix, weights):
    node_count = basis_matrix.shape[0] * lax.axis_size(NODES)
    vector_count = samples.shape[0] * lax.axis_size(DP)
    blocks, start = [], 0
    for rows in CHUNKS:
        blocks.append(basis_matrix[start : start + rows])
        start += rows

    chips, crossed = [], []
    for block in blocks:
        partial = dot(block, weights)
        chips.append(chip_sum(partial))
        crossed.append(swapped(chips[-1], "y_lo"))

    centres, scores, tops, shift = [], [], [], None
    for chip, arrived in zip(chips, crossed):
        centre = whole_sum(chip, arrived)
        if shift is None:
            shift = jnp.mean(centre, axis=0, keepdims=True)
        cross = dot(centre - shift, samples, 1, 1)
        scores.append(inverse_temp * (cross - 0.5 * jnp.sum(centre * centre, axis=1)[:, None]))
        tops.append(jnp.max(scores[-1], axis=0))
        centres.append(centre)
    local_max = tops[0]
    for top in tops[1:]:
        local_max = jnp.maximum(local_max, top)
    exponents = [jnp.exp(part - local_max[None, :]) for part in scores]
    local_total = sum(jnp.sum(part, axis=0) for part in exponents)
    common = inverse_temp * jnp.sum(samples * shift, axis=1)
    shifted_max = local_max + common
    maxima, totals = over_nodes(jnp.stack([shifted_max, local_total]))
    factor = jnp.exp(shifted_max - maxima) / totals

    chips, crossed = [], []
    for centre, exponent in zip(centres, exponents):
        resp = exponent * factor[None, :]
        terms = jnp.sum(resp, axis=1)[:, None] * centre - dot(resp, samples)
        chips.append(chip_sum(terms))
        crossed.append(swapped(chips[-1], "y_lo"))
    partial_gradient = 0.0
    for block, chip, arrived in zip(blocks, chips, crossed):
        terms = whole_sum(chip, arrived)
        partial_gradient += dot(block, terms, 0, 0)

    step_rate = 8.0 * math.sqrt(node_count) / vector_count
    gradient_rows = scattered(scattered(partial_gradient, "x"), "z")
    gradient_rows = gradient_rows + swapped(gradient_rows, "y_hi")
    row_count = gradient_rows.shape[0]
    place = lax.axis_index(("x", "z")) * row_count
    own_rows = lax.dynamic_slice_in_dim(weights, place, row_count, 0)
    updated = shrink * own_rows - step_rate * gradient_rows
    new_weights = gathered(gathered(updated, "z"), "x")
    chips, crossed = [], []
    for block in blocks:
        partial = dot(block, new_weights)
        chips.append(chip_sum(partial))
        crossed.append(swapped(chips[-1], "y_lo"))
    new_centres = jnp.concatenate([whole_sum(*pair) for pair in zip(chips, crossed)])
    return (new_weights, new_centres)


def solution(mesh):
    split = Mesh(mesh.devices.reshape(4, 8, 2, 2, 2), NODES + DP)
    placed = (P(DP, None), P(NODES, DP), P(DP, None))
    return jax.shard_map(
        step,
        mesh=split,
        in_specs=placed,
        out_specs=(P(DP, None), P(NODES, None)),
        check_vma=False,
    )
```

```python
import math

import jax
import jax.numpy as jnp
from jax import lax
from jax.sharding import Mesh
from jax.sharding import PartitionSpec as P


NODES = ("x", "z", "y_hi")
DP = ("y_lo", "core")
CHUNKS = (256, 384, 384)

three_pass = lax.Precision.HIGH
inverse_temp = 0.25
shrink = 0.95


def swapped(array, axis):
    return lax.ppermute(array, axis, [(0, 1), (1, 0)])


def dot(first, second, first_dim=1, second_dim=0, precision=three_pass):
    return lax.dot_general(
        first,
        second,
        (((first_dim,), (second_dim,)), ((), ())),
        precision=precision,
        preferred_element_type=jnp.float32,
    )


def chip_sum(partial):
    half = partial.shape[0] // 2
    first = lax.axis_index("core") == 0
    top, bottom = partial[:half], partial[half:]
    mine, other = jnp.where(first, top, bottom), jnp.where(first, bottom, top)
    return mine + swapped(other, "core")


def whole_sum(chip, arrived):
    first = lax.axis_index("core") == 0
    full = chip + arrived
    sibling = swapped(full, "core")
    return jnp.concatenate([jnp.where(first, full, sibling), jnp.where(first, sibling, full)])


def merged(*stats):
    top = stats[0][0]
    for other in stats[1:]:
        top = jnp.maximum(top, other[0])
    total = sum(other[1] * jnp.exp(other[0] - top) for other in stats)
    return jnp.stack([top, total])


def moved(array, axis, where):
    count = lax.axis_size(axis)
    return lax.ppermute(array, axis, [(k, where(k) % count) for k in range(count)])


def over_nodes(stats):
    others = [moved(stats, "x", lambda k, d=d: k + d) for d in (1, 3, 2)]
    stats = merged(stats, *others)
    for flip in (1, 3, 7):
        stats = merged(stats, moved(stats, "z", lambda k: k ^ flip))
    return merged(stats, swapped(stats, "y_hi"))


def scattered(array, axis):
    parts = array.reshape(lax.axis_size(axis), -1, array.shape[1])
    return lax.all_to_all(parts, axis, 0, 0, tiled=True).sum(axis=0)


def gathered(array, axis):
    spread = jnp.broadcast_to(array[None], (lax.axis_size(axis), *array.shape))
    return lax.all_to_all(spread, axis, 0, 0, tiled=True).reshape(-1, array.shape[1])


def gathered_by_permute(array, axis):
    count, place = lax.axis_size(axis), lax.axis_index(axis)
    arrived = [(d, moved(array, axis, lambda k, d=d: k + d)) for d in (1, 3, 2)]
    whole = jnp.zeros((count, *array.shape), array.dtype)
    for d, block in [(0, array), *arrived]:
        whole = lax.dynamic_update_index_in_dim(whole, block, (place - d) % count, 0)
    return whole.reshape(-1, array.shape[1])


def step(samples, basis_matrix, weights):
    node_count = basis_matrix.shape[0] * lax.axis_size(NODES)
    vector_count = samples.shape[0] * lax.axis_size(DP)
    blocks, start = [], 0
    for rows in CHUNKS:
        blocks.append(basis_matrix[start : start + rows])
        start += rows

    chips, crossed = [], []
    for block in blocks:
        partial = dot(block, weights)
        chips.append(chip_sum(partial))
        crossed.append(swapped(chips[-1], "y_lo"))

    centres, scores, tops, shift = [], [], [], None
    for chip, arrived in zip(chips, crossed):
        centre = whole_sum(chip, arrived)
        if shift is None:
            shift = jnp.mean(centre, axis=0, keepdims=True)
        cross = dot(centre - shift, samples, 1, 1)
        scores.append(inverse_temp * (cross - 0.5 * jnp.sum(centre * centre, axis=1)[:, None]))
        tops.append(jnp.max(scores[-1], axis=0))
        centres.append(centre)
    local_max = tops[0]
    for top in tops[1:]:
        local_max = jnp.maximum(local_max, top)
    exponents = [jnp.exp(part - local_max[None, :]) for part in scores]
    local_total = sum(jnp.sum(part, axis=0) for part in exponents)
    common = inverse_temp * jnp.sum(samples * shift, axis=1)
    shifted_max = local_max + common
    maxima, totals = over_nodes(jnp.stack([shifted_max, local_total]))
    factor = jnp.exp(shifted_max - maxima) / totals

    chips, crossed = [], []
    for centre, exponent in zip(centres, exponents):
        resp = exponent * factor[None, :]
        terms = jnp.sum(resp, axis=1)[:, None] * centre - dot(resp, samples)
        chips.append(chip_sum(terms))
        crossed.append(swapped(chips[-1], "y_lo"))
    partial_gradient = 0.0
    for block, chip, arrived in zip(blocks, chips, crossed):
        terms = whole_sum(chip, arrived)
        partial_gradient = lax.optimization_barrier(partial_gradient + dot(block, terms, 0, 0))

    step_rate = 8.0 * math.sqrt(node_count) / vector_count
    gradient_rows = scattered(scattered(partial_gradient, "x"), "z")
    gradient_rows = gradient_rows + swapped(gradient_rows, "y_hi")
    row_count = gradient_rows.shape[0]
    place = lax.axis_index(("x", "z")) * row_count
    own_rows = lax.dynamic_slice_in_dim(weights, place, row_count, 0)
    updated = shrink * own_rows - step_rate * gradient_rows
    new_weights = gathered_by_permute(gathered(updated, "z"), "x")
    chips, crossed = [], []
    for block in blocks:
        partial = dot(block, new_weights)
        chips.append(chip_sum(partial))
        crossed.append(swapped(chips[-1], "y_lo"))
    new_centres = jnp.concatenate([whole_sum(*pair) for pair in zip(chips, crossed)])
    return (new_weights, new_centres)


def solution(mesh):
    split = Mesh(mesh.devices.reshape(4, 8, 2, 2, 2), NODES + DP)
    placed = (P(DP, None), P(NODES, DP), P(DP, None))
    return jax.shard_map(
        step,
        mesh=split,
        in_specs=placed,
        out_specs=(P(DP, None), P(NODES, None)),
        check_vma=False,
    )
```

```python
import math

import jax
import jax.numpy as jnp
from jax import lax
from jax.sharding import Mesh
from jax.sharding import PartitionSpec as P


NODES = ("x", "z", "y_hi")
DP = ("y_lo", "core")
CHUNKS = (256, 384, 384)

three_pass = lax.Precision.HIGH
inverse_temp = 0.25
shrink = 0.95


def swapped(array, axis):
    return lax.ppermute(array, axis, [(0, 1), (1, 0)])


def dot(first, second, first_dim=1, second_dim=0, precision=three_pass):
    return lax.dot_general(
        first,
        second,
        (((first_dim,), (second_dim,)), ((), ())),
        precision=precision,
        preferred_element_type=jnp.float32,
    )


def chip_sum(partial):
    half = partial.shape[0] // 2
    first = lax.axis_index("core") == 0
    top, bottom = partial[:half], partial[half:]
    mine, other = jnp.where(first, top, bottom), jnp.where(first, bottom, top)
    return mine + swapped(other, "core")


def whole_sum(chip, arrived):
    first = lax.axis_index("core") == 0
    full = chip + arrived
    sibling = swapped(full, "core")
    return jnp.concatenate([jnp.where(first, full, sibling), jnp.where(first, sibling, full)])


def merged(*stats):
    top = stats[0][0]
    for other in stats[1:]:
        top = jnp.maximum(top, other[0])
    total = sum(other[1] * jnp.exp(other[0] - top) for other in stats)
    return jnp.stack([top, total])


def moved(array, axis, where):
    count = lax.axis_size(axis)
    return lax.ppermute(array, axis, [(k, where(k) % count) for k in range(count)])


def over_nodes(stats):
    others = [moved(stats, "x", lambda k, d=d: k + d) for d in (1, 3, 2)]
    stats = merged(stats, *others)
    for flip in (1, 3, 7):
        stats = merged(stats, moved(stats, "z", lambda k: k ^ flip))
    return merged(stats, swapped(stats, "y_hi"))


def scattered(array, axis):
    parts = array.reshape(lax.axis_size(axis), -1, array.shape[1])
    return lax.all_to_all(parts, axis, 0, 0, tiled=True).sum(axis=0)


def gathered(array, axis):
    spread = jnp.broadcast_to(array[None], (lax.axis_size(axis), *array.shape))
    return lax.all_to_all(spread, axis, 0, 0, tiled=True).reshape(-1, array.shape[1])


def scattered_by_permute(array, axis):
    count, place = lax.axis_size(axis), lax.axis_index(axis)
    rows = array.shape[0] // count

    def block(k):
        return lax.dynamic_slice_in_dim(array, (place + k) % count * rows, rows, 0)

    arrived = [moved(block(d), axis, lambda k, d=d: k + d) for d in (1, 3, 2)]
    return block(0) + sum(arrived)


def gathered_by_permute(array, axis):
    count, place = lax.axis_size(axis), lax.axis_index(axis)
    arrived = [(d, moved(array, axis, lambda k, d=d: k + d)) for d in (1, 3, 2)]
    whole = jnp.zeros((count * array.shape[0], array.shape[1]), array.dtype)
    for d, block in [(0, array), *arrived]:
        start = (place - d) % count * array.shape[0]
        whole = lax.dynamic_update_slice_in_dim(whole, block, start, 0)
    return whole


def step(samples, basis_matrix, weights):
    node_count = basis_matrix.shape[0] * lax.axis_size(NODES)
    vector_count = samples.shape[0] * lax.axis_size(DP)
    blocks, start = [], 0
    for rows in CHUNKS:
        blocks.append(basis_matrix[start : start + rows])
        start += rows

    chips, crossed = [], []
    for block in blocks:
        partial = dot(block, weights)
        chips.append(chip_sum(partial))
        crossed.append(swapped(chips[-1], "y_lo"))

    centres, scores, tops, shift = [], [], [], None
    for chip, arrived in zip(chips, crossed):
        centre = whole_sum(chip, arrived)
        if shift is None:
            shift = jnp.mean(centre, axis=0, keepdims=True)
        cross = dot(centre - shift, samples, 1, 1)
        scores.append(inverse_temp * (cross - 0.5 * jnp.sum(centre * centre, axis=1)[:, None]))
        tops.append(jnp.max(scores[-1], axis=0))
        centres.append(centre)
    local_max = tops[0]
    for top in tops[1:]:
        local_max = jnp.maximum(local_max, top)
    exponents = [jnp.exp(part - local_max[None, :]) for part in scores]
    local_total = sum(jnp.sum(part, axis=0) for part in exponents)
    common = inverse_temp * jnp.sum(samples * shift, axis=1)
    shifted_max = local_max + common
    maxima, totals = over_nodes(jnp.stack([shifted_max, local_total]))
    factor = jnp.exp(shifted_max - maxima) / totals

    chips, crossed = [], []
    for centre, exponent in zip(centres, exponents):
        resp = exponent * factor[None, :]
        terms = jnp.sum(resp, axis=1)[:, None] * centre - dot(resp, samples)
        chips.append(chip_sum(terms))
        crossed.append(swapped(chips[-1], "y_lo"))
    partial_gradient = 0.0
    for block, chip, arrived in zip(blocks, chips, crossed):
        terms = whole_sum(chip, arrived)
        partial_gradient = lax.optimization_barrier(partial_gradient + dot(block, terms, 0, 0))

    step_rate = 8.0 * math.sqrt(node_count) / vector_count
    gradient_rows = scattered(scattered_by_permute(partial_gradient, "x"), "z")
    gradient_rows = gradient_rows + swapped(gradient_rows, "y_hi")
    row_count = gradient_rows.shape[0]
    place = lax.axis_index(("x", "z")) * row_count
    own_rows = lax.dynamic_slice_in_dim(weights, place, row_count, 0)
    updated = shrink * own_rows - step_rate * gradient_rows
    new_weights = gathered_by_permute(gathered(updated, "z"), "x")
    chips, crossed = [], []
    for block in blocks:
        partial = dot(block, new_weights)
        chips.append(chip_sum(partial))
        crossed.append(swapped(chips[-1], "y_lo"))
    new_centres = jnp.concatenate([whole_sum(*pair) for pair in zip(chips, crossed)])
    return (new_weights, new_centres)


def solution(mesh):
    split = Mesh(mesh.devices.reshape(4, 8, 2, 2, 2), NODES + DP)
    placed = (P(DP, None), P(NODES, DP), P(DP, None))
    return jax.shard_map(
        step,
        mesh=split,
        in_specs=placed,
        out_specs=(P(DP, None), P(NODES, None)),
        check_vma=False,
    )
```
